1024 devices in a mesh: rows: 128 (over y, z), protos: 8 (over x, core).
Axes of the slice: x: 4, y: 8, z: 16, core: 2. Of those that a mesh axis runs over, the one named last changes fastest.
Arguments:
- features: bfloat16 [49152, 256], P('rows', 'protos'), may hold values from -12 to 12
- prototypes: bfloat16 [65536, 256], P('protos', 'rows'), may hold values from -8 to 8
- masked_index: int32 [24576], P('rows'), may hold values from 0 to 383
Outputs:
- targets: bfloat16 [24576, 65536], P('rows', 'protos')
The draws below stay inside these ranges and needn't reach their ends.
Inputs may be any that keep to these rules, and one draw needn't show every extreme that they name: Row r of the whole takes patch (r // 192) * 384 + masked_index[r] of features.
All inputs are finite; a program needn't handle non-finite values.
Results may differ from the reference program's by a relative error of at most 0.001.
Values may be sent and summed in bfloat16 or wider, within the bound.
No kernel may reach another device: no remote copies, remote signals or barrier semaphores. Data moves between devices by JAX's collectives and lax.ppermute only.
A program may use at most 64 MiB of HBM per device.

```python
import jax
import jax.numpy as jnp
from jax import lax

D = 256
K = 65536
MASKED_DEV = 192
ITERS = 3
PATCH_DEV = 384
MASKED = 24576
PATCHES = 49152


def common_directions(key):
    return jax.random.normal(jax.random.fold_in(key, 7), (16, D), jnp.float32)


def draw_features(key, part):
    directions = common_directions(key)
    own_key = jax.random.fold_in(key, 41)
    first, second, third, fourth = jax.random.split(own_key, 4)
    groups = PATCHES // PATCH_DEV
    shifts = jax.random.normal(second, (groups, D), jnp.float32)
    amount = jax.random.uniform(third, (groups, 1), jnp.float32, 0.2, 1.0)
    picked = jax.random.randint(fourth, (groups,), 0, 16)
    aligned = 0.7 * jnp.take(directions, picked, axis=0)
    base = jax.random.normal(first, (PATCHES, D), jnp.float32)
    offset = jnp.repeat(shifts * amount + aligned, PATCH_DEV, axis=0)
    return jnp.clip(base + offset, -12.0, 12.0).astype(jnp.bfloat16)


def draw_prototypes(key, part):
    directions = common_directions(key)
    own_key = jax.random.fold_in(key, 43)
    block_ids = jnp.arange(K, dtype=jnp.int32) * 16 // K
    aligned = 0.6 * jnp.take(directions, block_ids, axis=0)
    base = jax.random.normal(own_key, (K, D), jnp.float32)
    return jnp.clip(base + aligned, -8.0, 8.0).astype(jnp.bfloat16)


def touch_ends(values, stream_key, smallest, largest):
    index_at = [jax.random.randint(jax.random.fold_in(stream_key, axis), (), 0, length) for axis, length in enumerate(values.shape)]
    widest = values.shape.index(max(values.shape))
    neighbour = index_at[:widest] + [(index_at[widest] + 1) % values.shape[widest]] + index_at[widest + 1:]
    return values.at[tuple(index_at)].set(smallest).at[tuple(neighbour)].set(largest)


def setup_inputs(seed: int = 0) -> dict:
    seeds = jax.random.split(jax.random.key(seed), 4)
    return {
        "features": draw_features(jax.random.fold_in(seeds[3], 71), 0),
        "prototypes": draw_prototypes(jax.random.fold_in(seeds[3], 71), 0),
        "masked_index": touch_ends(jax.random.randint(seeds[2], (MASKED,), 0, PATCH_DEV), jax.random.fold_in(seeds[2], 1), 0, PATCH_DEV - 1).astype(jnp.int32),
    }


TEMP = 0.07
EPS = 1e-06

def reference(features, prototypes, masked_index):
    owner = jnp.arange(MASKED, dtype=jnp.int32) // MASKED_DEV
    rowids = (owner * PATCH_DEV + masked_index).astype(jnp.int32)
    selected = jnp.take(features, rowids, axis=0)
    feat_scale = lax.rsqrt(lax.optimization_barrier(jnp.sum(jnp.square(selected.astype(jnp.float32)), axis=1)) + EPS)
    proto_scale = lax.rsqrt(lax.optimization_barrier(jnp.sum(jnp.square(prototypes.astype(jnp.float32)), axis=1)) + EPS)
    blocks = MASKED // MASKED_DEV
    protos_t = prototypes.T

    def weights_of(index):
        start = (index * MASKED_DEV).astype(jnp.int32)
        part = lax.dynamic_slice_in_dim(selected, start, MASKED_DEV, 0)
        scale = lax.dynamic_slice_in_dim(feat_scale, start, MASKED_DEV, 0)
        raw = jnp.dot(part, protos_t, preferred_element_type=jnp.float32)
        return jnp.exp(raw * scale[:, None] * proto_scale[None, :] / TEMP)

    def first_pass(total, index):
        return (total + lax.optimization_barrier(jnp.sum(weights_of(index), axis=0)), None)
    indices = jnp.arange(blocks, dtype=jnp.int32)
    col_mass, unused = lax.scan(first_pass, jnp.zeros((K,), jnp.float32), indices)
    for step in range(ITERS):
        col_scale = 1.0 / (K * col_mass)
        if step + 1 < ITERS:

            def middle(total, index):
                block = weights_of(index)
                row_mass = jnp.dot(block, col_scale, precision=lax.Precision.HIGHEST)
                row_scale = 1.0 / (MASKED * row_mass)
                return (total + jnp.dot(row_scale, block, precision=lax.Precision.HIGHEST), None)
            col_mass, unused = lax.scan(middle, jnp.zeros((K,), jnp.float32), indices)
        else:

            def final(carry, index):
                block = weights_of(index)
                row_mass = jnp.dot(block, col_scale, precision=lax.Precision.HIGHEST)
                row_scale = 1.0 / (MASKED * row_mass)
                result = float(K) * float(MASKED) * row_scale[:, None] * block * col_scale[None, :]
                return (carry, result.astype(jnp.bfloat16))
            unused, outputs = lax.scan(final, jnp.zeros((), jnp.float32), indices)
    return outputs.reshape(MASKED, K)
```

```python
import jax
import jax.numpy as jnp
from jax import lax
from jax.sharding import Mesh
from jax.sharding import PartitionSpec as P

K = 65536
ITERS = 3
TEMP = 0.07
EPS = 1e-06
NY = 8


def exchange(value, axes):
    return lax.all_to_all(value, axes, split_axis=0, concat_axis=0, tiled=True)


def from_everyone(value, axes):
    copies = jnp.broadcast_to(value, (lax.axis_size(axes), *value.shape))
    return exchange(copies, axes)


def on_device(features, prototypes, masked_index):
    n = masked_index.shape[0]
    ny, nz, npr = lax.axis_size("y"), lax.axis_size("z"), lax.axis_size("p")
    total_rows = n * ny * nz
    k_out = prototypes.shape[0]
    k_own = k_out // ny
    picks = (lax.broadcasted_iota(jnp.int32, (features.shape[0], n), 0) == masked_index[None, :])
    chosen = lax.dot_general(
        features, picks.astype(jnp.bfloat16), (((0,), (0,)), ((), ())),
        preferred_element_type=jnp.float32,
    ).astype(jnp.bfloat16)
    slices = prototypes.T.reshape(2, ny, k_own).transpose(1, 0, 2)
    slices = jnp.broadcast_to(slices[:, None], (ny, nz, 2, k_own)).reshape(ny * nz, 2, k_own)
    protos = exchange(slices, ("y", "z")).reshape(-1, k_own)
    patches = from_everyone(chosen, ("y", "p")).reshape(ny, -1, n)
    every_proto = lax.all_gather(protos, "y")
    dim = patches.shape[1]

    feat_scale = lax.rsqrt(jnp.sum(jnp.square(patches.astype(jnp.float32)), axis=1) + EPS)
    proto_scale = lax.rsqrt(jnp.sum(jnp.square(protos.astype(jnp.float32)), axis=0) + EPS)
    raw = lax.dot_general(
        patches, protos, (((1,), (0,)), ((), ())), preferred_element_type=jnp.float32
    )
    weights = jnp.exp(raw * feat_scale[:, :, None] * proto_scale[None, None, :] / TEMP)

    row_scale = None
    for step in range(ITERS):
        scaled = weights if row_scale is None else weights * row_scale[:, :, None]
        col_part = jnp.sum(scaled, axis=(0, 1)).reshape(-1, 128)
        col_sum = jnp.sum(from_everyone(col_part, "z"), axis=0).reshape(k_own)
        col_scale = 1.0 / (K * col_sum)
        row_part = jnp.sum(weights * col_scale[None, None, :], axis=2)
        if step + 1 < ITERS:
            row_sum = jnp.sum(from_everyone(row_part, ("y", "p")), axis=0)
            row_scale = 1.0 / (total_rows * row_sum)
    sent = jnp.concatenate(
        [row_part, jnp.broadcast_to(col_scale[None], (ny, k_own))], axis=1)
    width = sent.shape[1]
    sent = jnp.broadcast_to(sent[:, None], (ny, npr, width)).reshape(ny * npr, width)
    got = exchange(sent, ("y", "p")).reshape(ny, npr, width)
    row_scale = 1.0 / (total_rows * jnp.sum(got[:, :, :n], axis=(0, 1)))
    me_p = lax.axis_index("p")
    me_y = lax.axis_index("y")
    col_all = lax.dynamic_index_in_dim(got, me_p, 1, keepdims=False)[:, n:]
    mine = lax.dynamic_index_in_dim(patches, me_y, 0, keepdims=False)
    mine_scale = lax.dynamic_index_in_dim(feat_scale, me_y, 0, keepdims=False)
    every_scale = lax.rsqrt(jnp.sum(jnp.square(every_proto.astype(jnp.float32)), axis=1) + EPS)
    raw_out = lax.dot_general(
        mine, every_proto, (((0,), (1,)), ((), ())), preferred_element_type=jnp.float32
    )
    w_out = jnp.exp(raw_out * mine_scale[:, None, None] * every_scale[None] / TEMP)
    factor = float(K) * float(total_rows)
    out = (factor * row_scale)[:, None, None] * w_out * col_all[None]
    return out.astype(jnp.bfloat16).reshape(n, k_out)


def solution(mesh):
    rows = mesh.shape["rows"]
    split = Mesh(mesh.devices.reshape(NY, rows // NY, mesh.shape["protos"]), ("y", "z", "p"))
    in_specs = (P(("y", "z"), "p"), P("p", ("y", "z")), P(("y", "z")))
    out_specs = P(("y", "z"), "p")
    return jax.shard_map(
        on_device, mesh=split, in_specs=in_specs, out_specs=out_specs, check_vma=False
    )
```

```python
import jax
import jax.numpy as jnp
from jax import lax
from jax.sharding import Mesh
from jax.sharding import PartitionSpec as P

K = 65536
ITERS = 3
TEMP = 0.07
EPS = 1e-06
NY = 8


def exchange(value, axes):
    return lax.all_to_all(value, axes, split_axis=0, concat_axis=0, tiled=True)


def from_everyone(value, axes):
    copies = jnp.broadcast_to(value, (lax.axis_size(axes), *value.shape))
    return exchange(copies, axes)


def on_device(features, prototypes, masked_index):
    n = masked_index.shape[0]
    ny, nz = lax.axis_size("y"), lax.axis_size("z")
    total_rows = n * ny * nz
    k_out = prototypes.shape[0]
    k_own = k_out // ny
    lanes = -(-n // 128) * 128
    dim = features.shape[1] * lax.axis_size("p")
    picks = lax.broadcasted_iota(jnp.int32, (features.shape[0], lanes), 0) == jnp.pad(
        masked_index, (0, lanes - n), constant_values=-1)[None, :]
    chosen = lax.dot_general(
        features, picks.astype(jnp.bfloat16), (((0,), (0,)), ((), ())),
        preferred_element_type=jnp.float32,
    ).astype(jnp.bfloat16)
    slices = prototypes.T.reshape(2, ny, k_own // lanes, lanes).transpose(1, 0, 2, 3)
    slices = slices.reshape(ny, -1, lanes)
    held = slices.shape[1]
    both = jnp.concatenate(
        [slices, jnp.broadcast_to(chosen[None], (ny, *chosen.shape))], axis=1)
    both = exchange(both, "y")
    patches = lax.all_gather(both[:, held:], "p")
    protos = both[:, :held].reshape(2 * ny, k_own)
    protos = from_everyone(protos, "z").reshape(nz, ny, 2, k_own)
    protos = protos.transpose(1, 0, 2, 3).reshape(dim, k_own)
    patches = patches.transpose(1, 0, 2, 3).reshape(ny, dim, lanes)[:, :, :n]
    every_proto = lax.all_gather(protos, "y")
    dim = patches.shape[1]

    feat_scale = lax.rsqrt(jnp.sum(jnp.square(patches.astype(jnp.float32)), axis=1) + EPS)
    proto_scale = lax.rsqrt(jnp.sum(jnp.square(protos.astype(jnp.float32)), axis=0) + EPS)
    raw = lax.dot_general(
        patches, protos, (((1,), (0,)), ((), ())), preferred_element_type=jnp.float32
    )
    weights = jnp.exp(raw * feat_scale[:, :, None] * proto_scale[None, None, :] / TEMP)

    row_scale = None
    for step in range(ITERS):
        scaled = weights if row_scale is None else weights * row_scale[:, :, None]
        col_part = jnp.sum(scaled, axis=(0, 1)).reshape(-1, 128)
        col_sum = jnp.sum(from_everyone(col_part, "z"), axis=0).reshape(k_own)
        col_scale = 1.0 / (K * col_sum)
        row_part = jnp.sum(weights * col_scale[None, None, :], axis=2)
        row_part = jnp.sum(from_everyone(row_part, "p"), axis=0)
        if step + 1 < ITERS:
            row_sum = jnp.sum(from_everyone(row_part, "y"), axis=0)
            row_scale = 1.0 / (total_rows * row_sum)
    sent = jnp.concatenate(
        [row_part, jnp.broadcast_to(col_scale[None], (ny, k_own))], axis=1)
    got = exchange(sent, "y")
    row_scale = 1.0 / (total_rows * jnp.sum(got[:, :n], axis=0))
    col_all = got[:, n:]
    me_y = lax.axis_index("y")
    mine = lax.dynamic_index_in_dim(patches, me_y, 0, keepdims=False)
    mine_scale = lax.dynamic_index_in_dim(feat_scale, me_y, 0, keepdims=False)
    every_scale = lax.rsqrt(jnp.sum(jnp.square(every_proto.astype(jnp.float32)), axis=1) + EPS)
    raw_out = lax.dot_general(
        mine, every_proto, (((0,), (1,)), ((), ())), preferred_element_type=jnp.float32
    )
    w_out = jnp.exp(raw_out * mine_scale[:, None, None] * every_scale[None] / TEMP)
    factor = float(K) * float(total_rows)
    out = (factor * row_scale)[:, None, None] * w_out * col_all[None]
    return out.astype(jnp.bfloat16).reshape(n, k_out)


def solution(mesh):
    rows = mesh.shape["rows"]
    split = Mesh(mesh.devices.reshape(NY, rows // NY, mesh.shape["protos"]), ("y", "z", "p"))
    in_specs = (P(("y", "z"), "p"), P("p", ("y", "z")), P(("y", "z")))
    out_specs = P(("y", "z"), "p")
    return jax.shard_map(
        on_device, mesh=split, in_specs=in_specs, out_specs=out_specs, check_vma=False
    )
```

```python
import functools

import jax
import jax.numpy as jnp
from jax import lax
from jax.experimental import pallas as pl
from jax.experimental.pallas import tpu as pltpu
from jax.sharding import Mesh
from jax.sharding import PartitionSpec as P


K = 65536
ITERS = 3
TEMP = 0.07
EPS = 1e-06
NY = 8
LANES = 128
VMEM = pl.BlockSpec(memory_space=pltpu.VMEM)
HIGHEST = lax.Precision.HIGHEST


def exchange(value, axes):
    return lax.all_to_all(value, axes, split_axis=0, concat_axis=0, tiled=True)


def from_everyone(value, axes):
    copies = jnp.broadcast_to(value, (lax.axis_size(axes), *value.shape))
    return exchange(copies, axes)


def call(body, out_shape, flops, moved, limit=20 * 2**20, **kwargs):
    return pl.pallas_call(
        body,
        out_shape=out_shape,
        cost_estimate=pl.CostEstimate(flops=flops, bytes_accessed=moved, transcendentals=0),
        compiler_params=pltpu.CompilerParams(vmem_limit_bytes=limit),
        **kwargs,
    )


def lane_sums(block):
    ones = jnp.ones((8, block.shape[1]), jnp.float32)
    return lax.dot_general(
        ones, block, (((1,), (1,)), ((), ())), precision=HIGHEST,
        preferred_element_type=jnp.float32,
    )[0:1]


def column_sum(block):
    rows, width = block.shape
    return jnp.sum(jnp.sum(block.reshape(rows // 8, 8, width), axis=0), axis=0, keepdims=True)


def block_weights(feat, protos, proto_scale, n):
    feat32 = feat.astype(jnp.float32)
    scale = lax.rsqrt(jnp.sum(feat32 * feat32, axis=0, keepdims=True) + EPS)
    scale = jnp.broadcast_to(scale, (8, scale.shape[1])).T[:n, 0:1]
    raw = lax.dot_general(
        feat.T[:n], protos, (((1,), (0,)), ((), ())), preferred_element_type=jnp.float32
    )
    return jnp.exp(raw * scale * proto_scale / TEMP)


def squared_scale(protos):
    wide = protos.astype(jnp.float32)
    return lax.rsqrt(jnp.sum(wide * wide, axis=0, keepdims=True) + EPS)


def weights_body(n, me, feats, protos, weights, col_part, mine):
    npr, ny = feats.shape[0], feats.shape[1]
    values = protos[...]
    proto_scale = squared_scale(values)
    total = jnp.zeros((1, values.shape[1]), jnp.float32)
    for y in range(ny):
        feat = feats[:, y].reshape(npr * feats.shape[2], feats.shape[3])
        block = block_weights(feat, values, proto_scale, n)
        weights[y] = block
        total = total + column_sum(block)
    for z in range(col_part.shape[0]):
        col_part[z] = total
    mine[...] = feats[:, me[0]].reshape(mine.shape)


def row_body(weights, parts, row_part, col_scale):
    total = parts[0]
    for z in range(1, parts.shape[0]):
        total = total + parts[z]
    scale = 1.0 / (K * total)
    col_scale[...] = scale
    ny, n, width = weights.shape
    room = row_part.shape[2] - n
    for y in range(ny):
        acc = weights[y, :, :LANES] * scale[:, :LANES]
        for at in range(LANES, width, LANES):
            acc = acc + weights[y, :, at : at + LANES] * scale[:, at : at + LANES]
        sums = jnp.concatenate([lane_sums(acc), jnp.zeros((1, room), jnp.float32)], axis=1)
        for p in range(row_part.shape[0]):
            row_part[p, y : y + 1, :] = sums


def col_body(total_rows, weights, parts, col_part):
    total = parts[0]
    for y in range(1, parts.shape[0]):
        total = total + parts[y]
    scale = 1.0 / (total_rows * total)
    ny, n, width = weights.shape
    flipped = scale.T
    acc = jnp.zeros((8, width), jnp.float32)
    for y in range(ny):
        block = weights[y] * flipped[:n, y : y + 1]
        acc = acc + jnp.sum(block.reshape(n // 8, 8, width), axis=0)
    total = jnp.sum(acc, axis=0, keepdims=True)
    for z in range(col_part.shape[0]):
        col_part[z] = total


def added(parts):
    total = parts[0]
    for k in range(1, parts.shape[0]):
        total = total + parts[k]
    return total


def relay_body(parts, copies):
    total = added(parts)
    for y in range(copies.shape[0]):
        copies[y] = total


def last_body(parts, col_scale, sent):
    total = added(parts)
    lanes = total.shape[1]
    for y in range(sent.shape[0]):
        sent[y, :, :lanes] = total[y : y + 1]
        sent[y, :, lanes:] = col_scale[...]


def targets_body(total_rows, mine, protos, got, out):
    y = pl.program_id(0)
    n, width = out.shape
    lanes = got.shape[2] - width
    total = got[0, :, :lanes]
    for k in range(1, got.shape[0]):
        total = total + got[k, :, :lanes]
    factor = float(K) * float(total_rows)
    scale = factor * (1.0 / (total_rows * total))
    scale = jnp.broadcast_to(scale, (8, lanes)).T[:n, 0:1]
    values = protos[0]
    block = block_weights(mine[...], values, squared_scale(values), n)
    out[...] = (scale * block * got[y][:, lanes:]).astype(jnp.bfloat16)


def on_device(features, prototypes, masked_index):
    n = masked_index.shape[0]
    ny, nz, npr = lax.axis_size("y"), lax.axis_size("z"), lax.axis_size("p")
    total_rows = n * ny * nz
    k_out = prototypes.shape[0]
    k_own = k_out // ny
    lanes = -(-n // LANES) * LANES
    dim = features.shape[1] * npr
    f32, bf16 = jnp.float32, jnp.bfloat16
    elements = ny * n * k_own

    picks = lax.broadcasted_iota(jnp.int32, (features.shape[0], lanes), 0) == jnp.pad(
        masked_index, (0, lanes - n), constant_values=-1)[None, :]
    chosen = lax.dot_general(
        features, picks.astype(bf16), (((0,), (0,)), ((), ())), preferred_element_type=f32
    ).astype(bf16)
    slices = prototypes.T.reshape(2, ny, k_own // lanes, lanes).transpose(1, 0, 2, 3)
    slices = slices.reshape(ny, -1, lanes)
    held = slices.shape[1]
    both = jnp.concatenate(
        [slices, jnp.broadcast_to(chosen[None], (ny, *chosen.shape))], axis=1)
    both = exchange(both, "y")
    patches = lax.all_gather(both[:, held:], "p")
    protos = from_everyone(both[:, :held].reshape(2 * ny, k_own), "z")
    protos = protos.reshape(nz, ny, 2, k_own).transpose(1, 0, 2, 3).reshape(dim, k_own)
    every_proto = lax.all_gather(protos, "y")

    weights, col_part, mine = call(
        functools.partial(weights_body, n),
        (
            jax.ShapeDtypeStruct((ny, n, k_own), f32),
            jax.ShapeDtypeStruct((nz, 1, k_own), f32),
            jax.ShapeDtypeStruct((dim, lanes), bf16),
        ),
        2 * elements * dim, 4 * elements,
        in_specs=[pl.BlockSpec(memory_space=pltpu.SMEM), VMEM, VMEM],
        out_specs=(VMEM, VMEM, VMEM),
    )(lax.axis_index("y").reshape(1), patches, protos)

    for step in range(ITERS):
        parts = exchange(col_part, "z")
        row_part, col_scale = call(
            row_body,
            (jax.ShapeDtypeStruct((npr, ny, lanes), f32), jax.ShapeDtypeStruct((1, k_own), f32)),
            2 * elements, 4 * elements,
            in_specs=[VMEM, VMEM], out_specs=(VMEM, VMEM),
        )(weights, parts)
        parts = exchange(row_part, "p")
        if step + 1 < ITERS:
            copies = call(
                relay_body, jax.ShapeDtypeStruct((ny, ny, lanes), f32),
                ny * ny * lanes, 8 * ny * ny * lanes, in_specs=[VMEM], out_specs=VMEM,
            )(parts)
            col_part = call(
                functools.partial(col_body, total_rows),
                jax.ShapeDtypeStruct((nz, 1, k_own), f32),
                2 * elements, 4 * elements,
                in_specs=[VMEM, VMEM], out_specs=VMEM,
            )(weights, exchange(copies, "y"))
    sent = call(
        last_body, jax.ShapeDtypeStruct((ny, 1, lanes + k_own), f32),
        ny * ny * lanes, 8 * ny * ny * lanes, in_specs=[VMEM, VMEM], out_specs=VMEM,
    )(parts, col_scale)
    return call(
        functools.partial(targets_body, total_rows),
        jax.ShapeDtypeStruct((n, k_out), bf16),
        2 * elements * dim, 6 * elements,
        grid=(ny,),
        in_specs=[VMEM, pl.BlockSpec((1, dim, k_own), lambda i: (i, 0, 0)), VMEM],
        out_specs=pl.BlockSpec((n, k_own), lambda i: (0, i)),
    )(mine, pltpu.with_memory_space_constraint(every_proto, pltpu.HBM), exchange(sent, "y"))


def solution(mesh):
    rows = mesh.shape["rows"]
    split = Mesh(mesh.devices.reshape(NY, rows // NY, mesh.shape["protos"]), ("y", "z", "p"))
    in_specs = (P(("y", "z"), "p"), P("p", ("y", "z")), P(("y", "z")))
    out_specs = P(("y", "z"), "p")
    return jax.shard_map(
        on_device, mesh=split, in_specs=in_specs, out_specs=out_specs, check_vma=False
    )
```

```python
import functools

import jax
import jax.numpy as jnp
from jax import lax
from jax.experimental import pallas as pl
from jax.experimental.pallas import tpu as pltpu
from jax.sharding import Mesh
from jax.sharding import PartitionSpec as P


K = 65536
ITERS = 3
TEMP = 0.07
EPS = 1e-06
NY = 8
LANES = 128
VMEM = pl.BlockSpec(memory_space=pltpu.VMEM)
HIGHEST = lax.Precision.HIGHEST


def exchange(value, axes):
    return lax.all_to_all(value, axes, split_axis=0, concat_axis=0, tiled=True)


def from_everyone(value, axes):
    copies = jnp.broadcast_to(value, (lax.axis_size(axes), *value.shape))
    return exchange(copies, axes)


def call(body, out_shape, flops, moved, limit=20 * 2**20, **kwargs):
    return pl.pallas_call(
        body,
        out_shape=out_shape,
        cost_estimate=pl.CostEstimate(flops=flops, bytes_accessed=moved, transcendentals=0),
        compiler_params=pltpu.CompilerParams(vmem_limit_bytes=limit),
        **kwargs,
    )


def lane_sums(block):
    ones = jnp.ones((8, block.shape[1]), jnp.float32)
    return lax.dot_general(
        ones, block, (((1,), (1,)), ((), ())), precision=HIGHEST,
        preferred_element_type=jnp.float32,
    )[0:1]


def squared_scale(protos):
    wide = protos.astype(jnp.float32)
    return lax.rsqrt(jnp.sum(wide * wide, axis=0, keepdims=True) + EPS)


def block_weights(feat, feat_scale, protos):
    proto_scale = squared_scale(protos)
    raw = lax.dot_general(
        feat, protos, (((1,), (0,)), ((), ())), preferred_element_type=jnp.float32
    )
    parts = []
    for at in range(0, raw.shape[1], LANES):
        part = raw[:, at : at + LANES] * feat_scale * proto_scale[:, at : at + LANES]
        parts.append(jnp.exp(part / TEMP))
    return jnp.concatenate(parts, axis=1)


def feats_body(me, patches, feats, scales, mine, mine_scale):
    npr, ny, share, lanes = patches.shape
    n = feats.shape[1]
    for y in range(ny):
        feat = patches[:, y].reshape(npr * share, lanes)
        scale = jnp.broadcast_to(squared_scale(feat), (LANES, lanes)).T
        feats[y] = feat.T[:n]
        scales[y] = scale[:n]
    mine[...] = feats[me[0]]
    mine_scale[...] = scales[me[0]]


def weights_body(feats, scales, protos, weights, col_part):
    values = protos[...]
    total = jnp.zeros((8, values.shape[1]), jnp.float32)
    for y in range(feats.shape[0]):
        block = block_weights(feats[y], scales[y], values)
        weights[y] = block
        total = total + jnp.sum(block.reshape(-1, 8, block.shape[1]), axis=0)
    total = jnp.sum(total, axis=0, keepdims=True)
    for z in range(col_part.shape[0]):
        col_part[z] = total


def row_body(weights, parts, row_part, col_scale):
    total = parts[0]
    for z in range(1, parts.shape[0]):
        total = total + parts[z]
    scale = 1.0 / (K * total)
    col_scale[...] = scale
    ny, n, width = weights.shape
    room = row_part.shape[2] - n
    for y in range(ny):
        acc = weights[y, :, :LANES] * scale[:, :LANES]
        for at in range(LANES, width, LANES):
            acc = acc + weights[y, :, at : at + LANES] * scale[:, at : at + LANES]
        sums = jnp.concatenate([lane_sums(acc), jnp.zeros((1, room), jnp.float32)], axis=1)
        for p in range(row_part.shape[0]):
            row_part[p, y : y + 1, :] = sums


def col_body(total_rows, weights, parts, col_part):
    total = parts[0]
    for y in range(1, parts.shape[0]):
        total = total + parts[y]
    scale = 1.0 / (total_rows * total)
    ny, n, width = weights.shape
    flipped = scale.T
    acc = jnp.zeros((8, width), jnp.float32)
    for y in range(ny):
        block = weights[y] * flipped[:n, y : y + 1]
        acc = acc + jnp.sum(block.reshape(n // 8, 8, width), axis=0)
    total = jnp.sum(acc, axis=0, keepdims=True)
    for z in range(col_part.shape[0]):
        col_part[z] = total


def added(parts):
    total = parts[0]
    for k in range(1, parts.shape[0]):
        total = total + parts[k]
    return total


def relay_body(parts, copies):
    total = added(parts)
    for y in range(copies.shape[0]):
        copies[y] = total


def last_body(parts, col_scale, every_proto, sent):
    total = added(parts)
    lanes = total.shape[1]
    for y in range(sent.shape[0]):
        sent[y, :, :lanes] = total[y : y + 1]
        sent[y, :, lanes:] = col_scale[...]


def targets_body(total_rows, mine, mine_scale, protos, got, out):
    y = pl.program_id(0)
    n, width = out.shape
    lanes = got.shape[2] - width
    total = got[0, :, :lanes]
    for k in range(1, got.shape[0]):
        total = total + got[k, :, :lanes]
    factor = float(K) * float(total_rows)
    scale = factor * (1.0 / (total_rows * total))
    scale = jnp.broadcast_to(scale, (8, lanes)).T[:n, 0:1]
    block = block_weights(mine[...], mine_scale[...], protos[y])
    out[...] = (scale * block * got[y][:, lanes:]).astype(jnp.bfloat16)


def on_device(features, prototypes, masked_index):
    n = masked_index.shape[0]
    ny, nz, npr = lax.axis_size("y"), lax.axis_size("z"), lax.axis_size("p")
    total_rows = n * ny * nz
    k_out = prototypes.shape[0]
    k_own = k_out // ny
    lanes = -(-n // LANES) * LANES
    dim = features.shape[1] * npr
    f32, bf16 = jnp.float32, jnp.bfloat16
    elements = ny * n * k_own

    picks = lax.broadcasted_iota(jnp.int32, (features.shape[0], lanes), 0) == jnp.pad(
        masked_index, (0, lanes - n), constant_values=-1)[None, :]
    chosen = lax.dot_general(
        features, picks.astype(bf16), (((0,), (0,)), ((), ())), preferred_element_type=f32
    ).astype(bf16)
    slices = prototypes.T.reshape(2, ny, k_own // lanes, lanes).transpose(1, 0, 2, 3)
    slices = slices.reshape(ny, -1, lanes)
    held = slices.shape[1]
    both = jnp.concatenate(
        [slices, jnp.broadcast_to(chosen[None], (ny, *chosen.shape))], axis=1)
    both = exchange(both, "y")
    patches = lax.all_gather(both[:, held:], "p")
    protos = from_everyone(both[:, :held].reshape(2 * ny, k_own), "z")
    prepared = call(
        feats_body,
        (
            jax.ShapeDtypeStruct((ny, n, dim), bf16),
            jax.ShapeDtypeStruct((ny, n, LANES), f32),
            jax.ShapeDtypeStruct((n, dim), bf16),
            jax.ShapeDtypeStruct((n, LANES), f32),
        ),
        2 * ny * lanes * dim, 4 * ny * lanes * dim,
        in_specs=[pl.BlockSpec(memory_space=pltpu.SMEM), VMEM],
        out_specs=(VMEM, VMEM, VMEM, VMEM),
    )(lax.axis_index("y").reshape(1), patches)
    protos = protos.reshape(nz, ny, 2, k_own).transpose(1, 0, 2, 3).reshape(dim, k_own)
    feats, scales, mine, mine_scale = prepared
    every_proto = lax.all_gather(protos, "y")
    weights, col_part = call(
        weights_body,
        (
            jax.ShapeDtypeStruct((ny, n, k_own), f32),
            jax.ShapeDtypeStruct((nz, 1, k_own), f32),
        ),
        2 * elements * dim, 4 * elements,
        in_specs=[VMEM, VMEM, VMEM], out_specs=(VMEM, VMEM),
    )(feats, scales, protos)

    for step in range(ITERS):
        parts = exchange(col_part, "z")
        row_part, col_scale = call(
            row_body,
            (jax.ShapeDtypeStruct((npr, ny, lanes), f32), jax.ShapeDtypeStruct((1, k_own), f32)),
            2 * elements, 4 * elements,
            in_specs=[VMEM, VMEM], out_specs=(VMEM, VMEM),
        )(weights, parts)
        parts = exchange(row_part, "p")
        if step + 1 < ITERS:
            copies = call(
                relay_body, jax.ShapeDtypeStruct((ny, ny, lanes), f32),
                ny * ny * lanes, 8 * ny * ny * lanes, in_specs=[VMEM], out_specs=VMEM,
            )(parts)
            col_part = call(
                functools.partial(col_body, total_rows),
                jax.ShapeDtypeStruct((nz, 1, k_own), f32),
                2 * elements, 4 * elements,
                in_specs=[VMEM, VMEM], out_specs=VMEM,
            )(weights, exchange(copies, "y"))
    sent = call(
        last_body, jax.ShapeDtypeStruct((ny, 1, lanes + k_own), f32),
        ny * ny * lanes, 8 * ny * ny * lanes, in_specs=[VMEM, VMEM, pl.BlockSpec(memory_space=pl.ANY)], out_specs=VMEM,
    )(parts, col_scale, pltpu.with_memory_space_constraint(every_proto, pltpu.HBM))
    return call(
        functools.partial(targets_body, total_rows),
        jax.ShapeDtypeStruct((n, k_out), bf16),
        2 * elements * dim, 6 * elements,
        grid=(ny,),
        in_specs=[VMEM, VMEM, VMEM, VMEM],
        out_specs=pl.BlockSpec((n, k_own), lambda i: (0, i)),
    )(mine, mine_scale, every_proto, exchange(sent, "y"))


def solution(mesh):
    rows = mesh.shape["rows"]
    split = Mesh(mesh.devices.reshape(NY, rows // NY, mesh.shape["protos"]), ("y", "z", "p"))
    in_specs = (P(("y", "z"), "p"), P("p", ("y", "z")), P(("y", "z")))
    out_specs = P(("y", "z"), "p")
    return jax.shard_map(
        on_device, mesh=split, in_specs=in_specs, out_specs=out_specs, check_vma=False
    )
```

```python
import functools

import jax
import jax.numpy as jnp
from jax import lax
from jax.experimental import pallas as pl
from jax.experimental.pallas import tpu as pltpu
from jax.sharding import Mesh
from jax.sharding import PartitionSpec as P


K = 65536
ITERS = 3
TEMP = 0.07
EPS = 1e-06
NY = 8
LANES = 128
VMEM = pl.BlockSpec(memory_space=pltpu.VMEM)


def exchange(value, axes):
    return lax.all_to_all(value, axes, split_axis=0, concat_axis=0, tiled=True)


def from_everyone(value, axes):
    copies = jnp.broadcast_to(value, (lax.axis_size(axes), *value.shape))
    return exchange(copies, axes)


def in_hbm(value):
    return pltpu.with_memory_space_constraint(value, pltpu.HBM)


def call(body, out_shape, flops, moved, limit=20 * 2**20, **kwargs):
    return pl.pallas_call(
        body,
        out_shape=out_shape,
        cost_estimate=pl.CostEstimate(flops=flops, bytes_accessed=moved, transcendentals=0),
        compiler_params=pltpu.CompilerParams(vmem_limit_bytes=limit),
        **kwargs,
    )


def lane_sums(block, lanes):
    empty = jnp.zeros((lanes - block.shape[0], block.shape[1]), jnp.float32)
    return jnp.sum(jnp.concatenate([block, empty], axis=0).T, axis=0, keepdims=True)


def first_body(features, protos, index, both):
    ny, rows, lanes = both.shape
    share, count = features.shape
    n = index.shape[1]
    index = jnp.concatenate([index[...], jnp.full((1, lanes - n), -1, jnp.int32)], axis=1)
    picks = lax.broadcasted_iota(jnp.int32, (count, lanes), 0) == index
    chosen = lax.dot_general(
        features[...], picks.astype(jnp.float32).astype(jnp.bfloat16),
        (((1,), (0,)), ((), ())), preferred_element_type=jnp.float32,
    ).astype(jnp.bfloat16)
    held = rows - share
    for y in range(ny):
        for at in range(0, held, 2):
            start = (y * held // 2 + at // 2) * lanes
            both[y, at : at + 2, :] = protos[:, start : start + lanes]
        both[y, held:, :] = chosen


def squared_scale(protos):
    wide = protos.astype(jnp.float32)
    return lax.rsqrt(jnp.sum(wide * wide, axis=0, keepdims=True) + EPS)


def block_weights(feat, feat_scale, protos):
    proto_scale = squared_scale(protos)
    raw = lax.dot_general(
        feat, protos, (((1,), (0,)), ((), ())), preferred_element_type=jnp.float32
    )
    parts = []
    for at in range(0, raw.shape[1], LANES):
        part = raw[:, at : at + LANES] * feat_scale * proto_scale[:, at : at + LANES]
        parts.append(jnp.exp(part / TEMP))
    return jnp.concatenate(parts, axis=1)


def arrival_order(ny, nz):
    dim = 2 * ny * nz
    at = lax.broadcasted_iota(jnp.int32, (dim, dim), 0)
    low, mid = at & 1, (at >> 1) & (nz - 1)
    high = at >> nz.bit_length()
    target = mid * (2 * ny) + high * 2 + low
    hit = lax.broadcasted_iota(jnp.int32, (dim, dim), 1) == target
    return hit.astype(jnp.float32).astype(jnp.bfloat16)


def feats_body(nz, me, patches, feats, scales, mine, mine_scale):
    npr, ny, share, lanes = patches.shape
    n = feats.shape[1]
    order = arrival_order(ny, nz)
    for y in range(ny):
        feat = patches[:, y].reshape(npr * share, lanes)
        scales[y] = jnp.broadcast_to(squared_scale(feat), (LANES, lanes)).T[:n]
        feats[y] = lax.dot_general(
            feat.T[:n], order, (((1,), (0,)), ((), ())), preferred_element_type=jnp.float32
        ).astype(jnp.bfloat16)
    mine[...] = feats[me[0]]
    mine_scale[...] = scales[me[0]]


def weights_body(feats, scales, protos, weights, col_part):
    values = protos[...]
    total = jnp.zeros((8, values.shape[1]), jnp.float32)
    for y in range(feats.shape[0]):
        block = block_weights(feats[y], scales[y], values)
        weights[y] = block
        total = total + jnp.sum(block.reshape(-1, 8, block.shape[1]), axis=0)
    total = jnp.sum(total, axis=0, keepdims=True)
    for z in range(col_part.shape[0]):
        col_part[z] = total


def row_body(weights, parts, row_part, col_scale):
    total = parts[0]
    for z in range(1, parts.shape[0]):
        total = total + parts[z]
    scale = 1.0 / (K * total)
    col_scale[...] = scale
    ny, _, width = weights.shape
    for y in range(ny):
        acc = weights[y, :, :LANES] * scale[:, :LANES]
        for at in range(LANES, width, LANES):
            acc = acc + weights[y, :, at : at + LANES] * scale[:, at : at + LANES]
        sums = lane_sums(acc, row_part.shape[2])
        for p in range(row_part.shape[0]):
            row_part[p, y : y + 1, :] = sums


def col_body(total_rows, weights, parts, col_part):
    total = parts[0]
    for y in range(1, parts.shape[0]):
        total = total + parts[y]
    scale = 1.0 / (total_rows * total)
    ny, n, width = weights.shape
    flipped = scale.T
    acc = jnp.zeros((8, width), jnp.float32)
    for y in range(ny):
        block = weights[y] * flipped[:n, y : y + 1]
        acc = acc + jnp.sum(block.reshape(n // 8, 8, width), axis=0)
    total = jnp.sum(acc, axis=0, keepdims=True)
    for z in range(col_part.shape[0]):
        col_part[z] = total


def added(parts):
    total = parts[0]
    for k in range(1, parts.shape[0]):
        total = total + parts[k]
    return total


def relay_body(parts, copies):
    total = added(parts)
    for y in range(copies.shape[0]):
        copies[y] = total


def last_body(parts, col_scale, every_proto, sent):
    total = added(parts)
    lanes = total.shape[1]
    for y in range(sent.shape[0]):
        sent[y, :, :lanes] = total[y : y + 1]
        sent[y, :, lanes:] = col_scale[...]


def targets_body(total_rows, mine, mine_scale, protos, got, out, row_scale):
    step = pl.program_id(0)
    n = out.shape[0]
    width = protos.shape[2]
    lanes = got.shape[2] - width

    @pl.when(step == 0)
    def _():
        total = got[0, :, :lanes]
        for k in range(1, got.shape[0]):
            total = total + got[k, :, :lanes]
        factor = float(K) * float(total_rows)
        scale = factor * (1.0 / (total_rows * total))
        row_scale[...] = jnp.broadcast_to(scale, (LANES, lanes)).T[:n]

    count = out.shape[1] // width
    for k in range(count):
        y = step * count + k
        block = block_weights(mine[...], mine_scale[...], protos[y])
        col_scale = got[y][:, lanes:]
        for at in range(0, width, LANES):
            part = row_scale[...] * block[:, at : at + LANES] * col_scale[:, at : at + LANES]
            out[:, k * width + at : k * width + at + LANES] = part.astype(jnp.bfloat16)


def on_device(features, prototypes, masked_index):
    n = masked_index.shape[0]
    ny, nz, npr = lax.axis_size("y"), lax.axis_size("z"), lax.axis_size("p")
    total_rows = n * ny * nz
    k_out = prototypes.shape[0]
    k_own = k_out // ny
    lanes = -(-n // LANES) * LANES
    dim = features.shape[1] * npr
    f32, bf16 = jnp.float32, jnp.bfloat16
    elements = ny * n * k_own

    share = features.shape[1]
    held = 2 * k_own // lanes
    both = call(
        first_body, jax.ShapeDtypeStruct((ny, held + share, lanes), bf16),
        2 * share * lanes * features.shape[0], 4 * ny * share * lanes,
        grid=(1,),
        in_specs=[
            pl.BlockSpec((share, features.shape[0]), lambda i: (0, 0)),
            pl.BlockSpec((2, k_out), lambda i: (0, 0)),
            pl.BlockSpec((1, n), lambda i: (0, 0)),
        ],
        out_specs=VMEM,
    )(in_hbm(features.T), in_hbm(prototypes.T), in_hbm(masked_index.reshape(1, n)))
    both = exchange(both, "y")
    pieces = both[:, :held].reshape(ny, held // 2, 2, lanes).transpose(0, 2, 1, 3)
    pieces = pieces.reshape(2 * ny, k_own)
    patches = lax.all_gather(both[:, held:], "p")
    protos = from_everyone(pieces, "z").reshape(dim, k_own)
    prepared = call(
        functools.partial(feats_body, nz),
        (
            jax.ShapeDtypeStruct((ny, n, dim), bf16),
            jax.ShapeDtypeStruct((ny, n, LANES), f32),
            jax.ShapeDtypeStruct((n, dim), bf16),
            jax.ShapeDtypeStruct((n, LANES), f32),
        ),
        2 * ny * lanes * dim, 4 * ny * lanes * dim,
        in_specs=[pl.BlockSpec(memory_space=pltpu.SMEM), VMEM],
        out_specs=(VMEM, VMEM, VMEM, VMEM),
    )(lax.axis_index("y").reshape(1), patches)
    feats, scales, mine, mine_scale = prepared
    every_proto = lax.all_gather(protos, "y")
    weights, col_part = call(
        weights_body,
        (
            jax.ShapeDtypeStruct((ny, n, k_own), f32),
            jax.ShapeDtypeStruct((nz, 1, k_own), f32),
        ),
        2 * elements * dim, 4 * elements,
        in_specs=[VMEM, VMEM, VMEM], out_specs=(VMEM, VMEM),
    )(feats, scales, protos)

    for step in range(ITERS):
        parts = exchange(col_part, "z")
        row_part, col_scale = call(
            row_body,
            (jax.ShapeDtypeStruct((npr, ny, lanes), f32), jax.ShapeDtypeStruct((1, k_own), f32)),
            2 * elements, 4 * elements,
            in_specs=[VMEM, VMEM], out_specs=(VMEM, VMEM),
        )(weights, parts)
        parts = exchange(row_part, "p")
        if step + 1 < ITERS:
            copies = call(
                relay_body, jax.ShapeDtypeStruct((ny, ny, lanes), f32),
                ny * ny * lanes, 8 * ny * ny * lanes, in_specs=[VMEM], out_specs=VMEM,
            )(parts)
            col_part = call(
                functools.partial(col_body, total_rows),
                jax.ShapeDtypeStruct((nz, 1, k_own), f32),
                2 * elements, 4 * elements,
                in_specs=[VMEM, VMEM], out_specs=VMEM,
            )(weights, exchange(copies, "y"))
    sent = call(
        last_body, jax.ShapeDtypeStruct((ny, 1, lanes + k_own), f32),
        ny * ny * lanes, 8 * ny * ny * lanes, in_specs=[VMEM, VMEM, pl.BlockSpec(memory_space=pl.ANY)], out_specs=VMEM,
    )(parts, col_scale, in_hbm(every_proto))
    return call(
        functools.partial(targets_body, total_rows),
        jax.ShapeDtypeStruct((n, k_out), bf16),
        2 * elements * dim, 6 * elements,
        grid=(ny // 2,),
        in_specs=[VMEM, VMEM, VMEM, VMEM],
        out_specs=pl.BlockSpec((n, 2 * k_own), lambda i: (0, i)),
        scratch_shapes=[pltpu.VMEM((n, LANES), f32)],
    )(mine, mine_scale, every_proto, exchange(sent, "y"))


def solution(mesh):
    rows = mesh.shape["rows"]
    split = Mesh(mesh.devices.reshape(NY, rows // NY, mesh.shape["protos"]), ("y", "z", "p"))
    in_specs = (P(("y", "z"), "p"), P("p", ("y", "z")), P(("y", "z")))
    out_specs = P(("y", "z"), "p")
    return jax.shard_map(
        on_device, mesh=split, in_specs=in_specs, out_specs=out_specs, check_vma=False
    )
```

```python
import functools

import jax
import jax.numpy as jnp
from jax import lax
from jax.experimental import pallas as pl
from jax.experimental.pallas import tpu as pltpu
from jax.sharding import Mesh
from jax.sharding import PartitionSpec as P


K = 65536
ITERS = 3
TEMP = 0.07
EPS = 1e-06
NY = 8
LANES = 128
VMEM = pl.BlockSpec(memory_space=pltpu.VMEM)


def exchange(value, axes):
    return lax.all_to_all(value, axes, split_axis=0, concat_axis=0, tiled=True)


def in_hbm(value):
    return pltpu.with_memory_space_constraint(value, pltpu.HBM)


def call(body, out_shape, flops, moved, limit=20 * 2**20, **kwargs):
    return pl.pallas_call(
        body,
        out_shape=out_shape,
        cost_estimate=pl.CostEstimate(flops=flops, bytes_accessed=moved, transcendentals=0),
        compiler_params=pltpu.CompilerParams(vmem_limit_bytes=limit),
        **kwargs,
    )


def lane_sums(block, lanes):
    empty = jnp.zeros((lanes - block.shape[0], block.shape[1]), jnp.float32)
    return jnp.sum(jnp.concatenate([block, empty], axis=0).T, axis=0, keepdims=True)


def first_body(features, protos, index, both):
    ny, rows, lanes = both.shape
    share, count = features.shape
    n = index.shape[1]
    index = jnp.concatenate([index[...], jnp.full((1, lanes - n), -1, jnp.int32)], axis=1)
    picks = lax.broadcasted_iota(jnp.int32, (count, lanes), 0) == index
    chosen = lax.dot_general(
        features[...], picks.astype(jnp.float32).astype(jnp.bfloat16),
        (((1,), (0,)), ((), ())), preferred_element_type=jnp.float32,
    ).astype(jnp.bfloat16)
    held = rows - share
    for y in range(ny):
        for at in range(0, held, 2):
            start = (y * held // 2 + at // 2) * lanes
            both[y, at : at + 2, :] = protos[:, start : start + lanes]
        both[y, held:, :] = chosen


def second_body(both, chosen, pieces):
    ny = both.shape[0]
    nz, _, _ = pieces.shape
    lanes = both.shape[2]
    held = both.shape[1] - chosen.shape[1]
    chosen[...] = both[:, held:, :]
    for y in range(ny):
        for at in range(0, held, 2):
            pair = both[y, at : at + 2, :]
            start = at // 2 * lanes
            for z in range(nz):
                pieces[z, 2 * y : 2 * y + 2, start : start + lanes] = pair


def keep_body(protos, kept):
    kept[...] = protos[...]


def squared_scale(protos):
    wide = protos.astype(jnp.float32)
    return lax.rsqrt(jnp.sum(wide * wide, axis=0, keepdims=True) + EPS)


def block_weights(feat, feat_scale, protos):
    proto_scale = squared_scale(protos)
    raw = lax.dot_general(
        feat, protos, (((1,), (0,)), ((), ())), preferred_element_type=jnp.float32
    )
    parts = []
    for at in range(0, raw.shape[1], LANES):
        part = raw[:, at : at + LANES] * feat_scale * proto_scale[:, at : at + LANES]
        parts.append(jnp.exp(part / TEMP))
    return jnp.concatenate(parts, axis=1)


def arrival_order(ny, nz):
    dim = 2 * ny * nz
    at = lax.broadcasted_iota(jnp.int32, (dim, dim), 0)
    low, mid = at & 1, (at >> 1) & (nz - 1)
    high = at >> nz.bit_length()
    target = mid * (2 * ny) + high * 2 + low
    hit = lax.broadcasted_iota(jnp.int32, (dim, dim), 1) == target
    return hit.astype(jnp.float32).astype(jnp.bfloat16)


def feats_body(nz, ny, me, patches, feats, scales, mine, mine_scale):
    npr, count, share, lanes = patches.shape
    n = feats.shape[1]
    step = pl.program_id(0)
    order = arrival_order(ny, nz)
    for k in range(count):
        y = step * count + k
        feat = patches[:, k].reshape(npr * share, lanes)
        scales[y] = jnp.broadcast_to(squared_scale(feat), (LANES, lanes)).T[:n]
        feats[y] = lax.dot_general(
            feat.T[:n], order, (((1,), (0,)), ((), ())), preferred_element_type=jnp.float32
        ).astype(jnp.bfloat16)

    @pl.when(step == pl.num_programs(0) - 1)
    def _():
        mine[...] = feats[me[0]]
        mine_scale[...] = scales[me[0]]


def weights_body(feats, scales, protos, weights, col_part):
    values = protos[...]
    total = jnp.zeros((8, values.shape[1]), jnp.float32)
    for y in range(feats.shape[0]):
        block = block_weights(feats[y], scales[y], values)
        weights[y] = block
        total = total + jnp.sum(block.reshape(-1, 8, block.shape[1]), axis=0)
    total = jnp.sum(total, axis=0, keepdims=True)
    for z in range(col_part.shape[0]):
        col_part[z] = total


def row_body(weights, parts, row_part, col_scale):
    total = parts[0]
    for z in range(1, parts.shape[0]):
        total = total + parts[z]
    scale = 1.0 / (K * total)
    col_scale[...] = scale
    ny, _, width = weights.shape
    for y in range(ny):
        acc = weights[y, :, :LANES] * scale[:, :LANES]
        for at in range(LANES, width, LANES):
            acc = acc + weights[y, :, at : at + LANES] * scale[:, at : at + LANES]
        sums = lane_sums(acc, row_part.shape[2])
        for p in range(row_part.shape[0]):
            row_part[p, y : y + 1, :] = sums


def col_body(total_rows, weights, parts, col_part):
    total = parts[0]
    for y in range(1, parts.shape[0]):
        total = total + parts[y]
    scale = 1.0 / (total_rows * total)
    ny, n, width = weights.shape
    flipped = scale.T
    acc = jnp.zeros((8, width), jnp.float32)
    for y in range(ny):
        block = weights[y] * flipped[:n, y : y + 1]
        acc = acc + jnp.sum(block.reshape(n // 8, 8, width), axis=0)
    total = jnp.sum(acc, axis=0, keepdims=True)
    for z in range(col_part.shape[0]):
        col_part[z] = total


def added(parts):
    total = parts[0]
    for k in range(1, parts.shape[0]):
        total = total + parts[k]
    return total


def relay_body(parts, copies):
    total = added(parts)
    for y in range(copies.shape[0]):
        copies[y] = total


def last_body(parts, col_scale, every_proto, sent):
    total = added(parts)
    lanes = total.shape[1]
    for y in range(sent.shape[0]):
        sent[y, :, :lanes] = total[y : y + 1]
        sent[y, :, lanes:] = col_scale[...]


def targets_body(total_rows, mine, mine_scale, protos, got, out, row_scale):
    step = pl.program_id(0)
    n = out.shape[0]
    width = protos.shape[2]
    lanes = got.shape[2] - width

    @pl.when(step == 0)
    def _():
        total = got[0, :, :lanes]
        for k in range(1, got.shape[0]):
            total = total + got[k, :, :lanes]
        factor = float(K) * float(total_rows)
        scale = factor * (1.0 / (total_rows * total))
        row_scale[...] = jnp.broadcast_to(scale, (LANES, lanes)).T[:n]

    count = out.shape[1] // width
    for k in range(count):
        y = step * count + k
        block = block_weights(mine[...], mine_scale[...], protos[y])
        col_scale = got[y][:, lanes:]
        for at in range(0, width, LANES):
            part = row_scale[...] * block[:, at : at + LANES] * col_scale[:, at : at + LANES]
            out[:, k * width + at : k * width + at + LANES] = part.astype(jnp.bfloat16)


def on_device(features, prototypes, masked_index):
    n = masked_index.shape[0]
    ny, nz, npr = lax.axis_size("y"), lax.axis_size("z"), lax.axis_size("p")
    total_rows = n * ny * nz
    k_out = prototypes.shape[0]
    k_own = k_out // ny
    lanes = -(-n // LANES) * LANES
    dim = features.shape[1] * npr
    f32, bf16 = jnp.float32, jnp.bfloat16
    elements = ny * n * k_own

    share = features.shape[1]
    held = 2 * k_own // lanes
    both = call(
        first_body, jax.ShapeDtypeStruct((ny, held + share, lanes), bf16),
        2 * share * lanes * features.shape[0], 4 * ny * share * lanes,
        grid=(1,),
        in_specs=[
            pl.BlockSpec((share, features.shape[0]), lambda i: (0, 0)),
            pl.BlockSpec((2, k_out), lambda i: (0, 0)),
            pl.BlockSpec((1, n), lambda i: (0, 0)),
        ],
        out_specs=VMEM,
    )(in_hbm(features.T), in_hbm(prototypes.T), in_hbm(masked_index.reshape(1, n)))
    both = exchange(both, "y")
    chosen, pieces = call(
        second_body,
        (
            jax.ShapeDtypeStruct((ny, share, lanes), bf16),
            jax.ShapeDtypeStruct((nz, 2 * ny, k_own), bf16),
        ),
        ny * share * lanes, 4 * dim * k_own,
        grid=(1,),
        in_specs=[VMEM],
        out_specs=(
            pl.BlockSpec((ny, share, lanes), lambda i: (0, 0, 0)),
            pl.BlockSpec((nz, 2 * ny, k_own), lambda i: (0, 0, 0)),
        ),
    )(both)
    patches = lax.all_gather(chosen, "p")
    protos = exchange(pieces, "z").reshape(dim, k_own)
    prepared = call(
        functools.partial(feats_body, nz, ny),
        (
            jax.ShapeDtypeStruct((ny, n, dim), bf16),
            jax.ShapeDtypeStruct((ny, n, LANES), f32),
            jax.ShapeDtypeStruct((n, dim), bf16),
            jax.ShapeDtypeStruct((n, LANES), f32),
        ),
        2 * ny * lanes * dim, 4 * ny * lanes * dim,
        grid=(2,),
        in_specs=[
            pl.BlockSpec(memory_space=pltpu.SMEM),
            pl.BlockSpec((npr, ny // 2, share, lanes), lambda i: (0, i, 0, 0)),
        ],
        out_specs=(VMEM, VMEM, VMEM, VMEM),
    )(lax.axis_index("y").reshape(1), in_hbm(patches))
    feats, scales, mine, mine_scale = prepared
    kept = call(
        keep_body, jax.ShapeDtypeStruct((dim, k_own), bf16), dim * k_own, 4 * dim * k_own,
        grid=(1,),
        in_specs=[VMEM],
        out_specs=pl.BlockSpec((dim, k_own), lambda i: (0, 0)),
    )(protos)
    every_proto = lax.all_gather(kept, "y")
    weights, col_part = call(
        weights_body,
        (
            jax.ShapeDtypeStruct((ny, n, k_own), f32),
            jax.ShapeDtypeStruct((nz, 1, k_own), f32),
        ),
        2 * elements * dim, 4 * elements,
        in_specs=[VMEM, VMEM, VMEM], out_specs=(VMEM, VMEM),
    )(feats, scales, protos)

    for step in range(ITERS):
        parts = exchange(col_part, "z")
        row_part, col_scale = call(
            row_body,
            (jax.ShapeDtypeStruct((npr, ny, lanes), f32), jax.ShapeDtypeStruct((1, k_own), f32)),
            2 * elements, 4 * elements,
            in_specs=[VMEM, VMEM], out_specs=(VMEM, VMEM),
        )(weights, parts)
        parts = exchange(row_part, "p")
        if step + 1 < ITERS:
            copies = call(
                relay_body, jax.ShapeDtypeStruct((ny, ny, lanes), f32),
                ny * ny * lanes, 8 * ny * ny * lanes, in_specs=[VMEM], out_specs=VMEM,
            )(parts)
            col_part = call(
                functools.partial(col_body, total_rows),
                jax.ShapeDtypeStruct((nz, 1, k_own), f32),
                2 * elements, 4 * elements,
                in_specs=[VMEM, VMEM], out_specs=VMEM,
            )(weights, exchange(copies, "y"))
    sent = call(
        last_body, jax.ShapeDtypeStruct((ny, 1, lanes + k_own), f32),
        ny * ny * lanes, 8 * ny * ny * lanes, in_specs=[VMEM, VMEM, pl.BlockSpec(memory_space=pl.ANY)], out_specs=VMEM,
    )(parts, col_scale, in_hbm(every_proto))
    return call(
        functools.partial(targets_body, total_rows),
        jax.ShapeDtypeStruct((n, k_out), bf16),
        2 * elements * dim, 6 * elements,
        grid=(ny // 2,),
        in_specs=[VMEM, VMEM, VMEM, VMEM],
        out_specs=pl.BlockSpec((n, 2 * k_own), lambda i: (0, i)),
        scratch_shapes=[pltpu.VMEM((n, LANES), f32)],
    )(mine, mine_scale, every_proto, exchange(sent, "y"))


def solution(mesh):
    rows = mesh.shape["rows"]
    split = Mesh(mesh.devices.reshape(NY, rows // NY, mesh.shape["protos"]), ("y", "z", "p"))
    in_specs = (P(("y", "z"), "p"), P("p", ("y", "z")), P(("y", "z")))
    out_specs = P(("y", "z"), "p")
    return jax.shard_map(
        on_device, mesh=split, in_specs=in_specs, out_specs=out_specs, check_vma=False
    )
```

```python
import functools

import jax
import jax.numpy as jnp
from jax import lax
from jax.experimental import pallas as pl
from jax.experimental.pallas import tpu as pltpu
from jax.sharding import Mesh
from jax.sharding import PartitionSpec as P


K = 65536
ITERS = 3
TEMP = 0.07
EPS = 1e-06
NY = 8
LANES = 128
VMEM = pl.BlockSpec(memory_space=pltpu.VMEM)


def exchange(value, axes):
    return lax.all_to_all(value, axes, split_axis=0, concat_axis=0, tiled=True)


def in_hbm(value):
    return pltpu.with_memory_space_constraint(value, pltpu.HBM)


def call(body, out_shape, flops, moved, limit=20 * 2**20, **kwargs):
    return pl.pallas_call(
        body,
        out_shape=out_shape,
        cost_estimate=pl.CostEstimate(flops=flops, bytes_accessed=moved, transcendentals=0),
        compiler_params=pltpu.CompilerParams(vmem_limit_bytes=limit),
        **kwargs,
    )


def lane_sums(block, lanes):
    empty = jnp.zeros((lanes - block.shape[0], block.shape[1]), jnp.float32)
    return jnp.sum(jnp.concatenate([block, empty], axis=0).T, axis=0, keepdims=True)


def first_body(features, protos, index, both):
    ny, rows, lanes = both.shape
    share, count = features.shape
    n = index.shape[1]
    index = jnp.concatenate([index[...], jnp.full((1, lanes - n), -1, jnp.int32)], axis=1)
    picks = lax.broadcasted_iota(jnp.int32, (count, lanes), 0) == index
    chosen = lax.dot_general(
        features[...], picks.astype(jnp.float32).astype(jnp.bfloat16),
        (((1,), (0,)), ((), ())), preferred_element_type=jnp.float32,
    ).astype(jnp.bfloat16)
    held = rows - share
    for y in range(ny):
        for at in range(0, held, 2):
            start = (y * held // 2 + at // 2) * lanes
            both[y, at : at + 2, :] = protos[:, start : start + lanes]
        both[y, held:, :] = chosen


def second_body(both, chosen, pieces):
    ny = both.shape[0]
    nz, _, _ = pieces.shape
    lanes = both.shape[2]
    held = both.shape[1] - chosen.shape[1]
    chosen[...] = both[:, held:, :]
    for y in range(ny):
        for at in range(0, held, 2):
            pair = both[y, at : at + 2, :]
            start = at // 2 * lanes
            for z in range(nz):
                pieces[z, 2 * y : 2 * y + 2, start : start + lanes] = pair


def keep_body(protos, kept, sem):
    copy = pltpu.make_async_copy(protos, kept, sem)
    copy.start()
    copy.wait()


def squared_scale(protos):
    wide = protos.astype(jnp.float32)
    return lax.rsqrt(jnp.sum(wide * wide, axis=0, keepdims=True) + EPS)


def block_weights(feat, feat_scale, protos):
    proto_scale = squared_scale(protos)
    raw = lax.dot_general(
        feat, protos, (((1,), (0,)), ((), ())), preferred_element_type=jnp.float32
    )
    parts = []
    for at in range(0, raw.shape[1], LANES):
        part = raw[:, at : at + LANES] * feat_scale * proto_scale[:, at : at + LANES]
        parts.append(jnp.exp(part / TEMP))
    return jnp.concatenate(parts, axis=1)


def arrival_order(ny, nz):
    dim = 2 * ny * nz
    at = lax.broadcasted_iota(jnp.int32, (dim, dim), 0)
    low, mid = at & 1, (at >> 1) & (nz - 1)
    high = at >> nz.bit_length()
    target = mid * (2 * ny) + high * 2 + low
    hit = lax.broadcasted_iota(jnp.int32, (dim, dim), 1) == target
    return hit.astype(jnp.float32).astype(jnp.bfloat16)


def feats_body(nz, ny, me, patches, feats, scales, mine, mine_scale):
    npr, count, share, lanes = patches.shape
    n = feats.shape[1]
    step = pl.program_id(0)
    order = arrival_order(ny, nz)
    for k in range(count):
        y = step * count + k
        feat = patches[:, k].reshape(npr * share, lanes)
        scales[y] = jnp.broadcast_to(squared_scale(feat), (LANES, lanes)).T[:n]
        feats[y] = lax.dot_general(
            feat.T[:n], order, (((1,), (0,)), ((), ())), preferred_element_type=jnp.float32
        ).astype(jnp.bfloat16)

    @pl.when(step == pl.num_programs(0) - 1)
    def _():
        mine[...] = feats[me[0]]
        mine_scale[...] = scales[me[0]]


def weights_body(feats, scales, protos, weights, col_part):
    values = protos[...]
    total = jnp.zeros((8, values.shape[1]), jnp.float32)
    for y in range(feats.shape[0]):
        block = block_weights(feats[y], scales[y], values)
        weights[y] = block
        total = total + jnp.sum(block.reshape(-1, 8, block.shape[1]), axis=0)
    total = jnp.sum(total, axis=0, keepdims=True)
    for z in range(col_part.shape[0]):
        col_part[z] = total


def row_body(weights, parts, row_part, col_scale):
    total = parts[0]
    for z in range(1, parts.shape[0]):
        total = total + parts[z]
    scale = 1.0 / (K * total)
    col_scale[...] = scale
    ny, _, width = weights.shape
    for y in range(ny):
        acc = weights[y, :, :LANES] * scale[:, :LANES]
        for at in range(LANES, width, LANES):
            acc = acc + weights[y, :, at : at + LANES] * scale[:, at : at + LANES]
        sums = lane_sums(acc, row_part.shape[2])
        for p in range(row_part.shape[0]):
            row_part[p, y : y + 1, :] = sums


def col_body(total_rows, weights, parts, col_part):
    total = parts[0]
    for y in range(1, parts.shape[0]):
        total = total + parts[y]
    scale = 1.0 / (total_rows * total)
    ny, n, width = weights.shape
    flipped = scale.T
    acc = jnp.zeros((8, width), jnp.float32)
    for y in range(ny):
        block = weights[y] * flipped[:n, y : y + 1]
        acc = acc + jnp.sum(block.reshape(n // 8, 8, width), axis=0)
    total = jnp.sum(acc, axis=0, keepdims=True)
    for z in range(col_part.shape[0]):
        col_part[z] = total


def added(parts):
    total = parts[0]
    for k in range(1, parts.shape[0]):
        total = total + parts[k]
    return total


def relay_body(parts, copies):
    total = added(parts)
    for y in range(copies.shape[0]):
        copies[y] = total


def last_body(parts, col_scale, every_proto, sent):
    total = added(parts)
    lanes = total.shape[1]
    for y in range(sent.shape[0]):
        sent[y, :, :lanes] = total[y : y + 1]
        sent[y, :, lanes:] = col_scale[...]


def targets_body(total_rows, mine, mine_scale, protos, got, out, slots, sems):
    count, n, width = slots.shape
    lanes = got.shape[2] - width
    total = got[0, :, :lanes]
    for k in range(1, got.shape[0]):
        total = total + got[k, :, :lanes]
    factor = float(K) * float(total_rows)
    scale = factor * (1.0 / (total_rows * total))
    scale = jnp.broadcast_to(scale, (LANES, lanes)).T[:n]
    copies = []
    for y in range(count):
        block = block_weights(mine[...], mine_scale[...], protos[y])
        col_scale = got[y][:, lanes:]
        for at in range(0, width, LANES):
            part = scale * block[:, at : at + LANES] * col_scale[:, at : at + LANES]
            slots[y, :, at : at + LANES] = part.astype(jnp.bfloat16)
        copy = pltpu.make_async_copy(
            slots.at[y], out.at[:, y * width : (y + 1) * width], sems.at[y]
        )
        copy.start()
        copies.append(copy)
    for copy in copies:
        copy.wait()


def on_device(features, prototypes, masked_index):
    n = masked_index.shape[0]
    ny, nz, npr = lax.axis_size("y"), lax.axis_size("z"), lax.axis_size("p")
    total_rows = n * ny * nz
    k_out = prototypes.shape[0]
    k_own = k_out // ny
    lanes = -(-n // LANES) * LANES
    dim = features.shape[1] * npr
    f32, bf16 = jnp.float32, jnp.bfloat16
    elements = ny * n * k_own

    share = features.shape[1]
    held = 2 * k_own // lanes
    both = call(
        first_body, jax.ShapeDtypeStruct((ny, held + share, lanes), bf16),
        2 * share * lanes * features.shape[0], 4 * ny * share * lanes,
        grid=(1,),
        in_specs=[
            pl.BlockSpec((share, features.shape[0]), lambda i: (0, 0)),
            pl.BlockSpec((2, k_out), lambda i: (0, 0)),
            pl.BlockSpec((1, n), lambda i: (0, 0)),
        ],
        out_specs=VMEM,
    )(in_hbm(features.T), in_hbm(prototypes.T), in_hbm(masked_index.reshape(1, n)))
    both = exchange(both, "y")
    chosen, pieces = call(
        second_body,
        (
            jax.ShapeDtypeStruct((ny, share, lanes), bf16),
            jax.ShapeDtypeStruct((nz, 2 * ny, k_own), bf16),
        ),
        ny * share * lanes, 4 * dim * k_own,
        grid=(1,),
        in_specs=[VMEM],
        out_specs=(
            pl.BlockSpec((ny, share, lanes), lambda i: (0, 0, 0)),
            pl.BlockSpec((nz, 2 * ny, k_own), lambda i: (0, 0, 0)),
        ),
    )(both)
    patches = lax.all_gather(chosen, "p")
    protos = exchange(pieces, "z").reshape(dim, k_own)
    prepared = call(
        functools.partial(feats_body, nz, ny),
        (
            jax.ShapeDtypeStruct((ny, n, dim), bf16),
            jax.ShapeDtypeStruct((ny, n, LANES), f32),
            jax.ShapeDtypeStruct((n, dim), bf16),
            jax.ShapeDtypeStruct((n, LANES), f32),
        ),
        2 * ny * lanes * dim, 4 * ny * lanes * dim,
        grid=(2,),
        in_specs=[
            pl.BlockSpec(memory_space=pltpu.SMEM),
            pl.BlockSpec((npr, ny // 2, share, lanes), lambda i: (0, i, 0, 0)),
        ],
        out_specs=(VMEM, VMEM, VMEM, VMEM),
    )(lax.axis_index("y").reshape(1), in_hbm(patches))
    feats, scales, mine, mine_scale = prepared
    kept = call(
        keep_body, jax.ShapeDtypeStruct((dim, k_own), bf16), dim * k_own, 4 * dim * k_own,
        in_specs=[VMEM],
        out_specs=pl.BlockSpec(memory_space=pltpu.HBM),
        scratch_shapes=[pltpu.SemaphoreType.DMA],
    )(protos)
    every_proto = lax.all_gather(kept, "y")
    weights, col_part = call(
        weights_body,
        (
            jax.ShapeDtypeStruct((ny, n, k_own), f32),
            jax.ShapeDtypeStruct((nz, 1, k_own), f32),
        ),
        2 * elements * dim, 4 * elements,
        in_specs=[VMEM, VMEM, VMEM], out_specs=(VMEM, VMEM),
    )(feats, scales, protos)

    for step in range(ITERS):
        parts = exchange(col_part, "z")
        row_part, col_scale = call(
            row_body,
            (jax.ShapeDtypeStruct((npr, ny, lanes), f32), jax.ShapeDtypeStruct((1, k_own), f32)),
            2 * elements, 4 * elements,
            in_specs=[VMEM, VMEM], out_specs=(VMEM, VMEM),
        )(weights, parts)
        parts = exchange(row_part, "p")
        if step + 1 < ITERS:
            copies = call(
                relay_body, jax.ShapeDtypeStruct((ny, ny, lanes), f32),
                ny * ny * lanes, 8 * ny * ny * lanes, in_specs=[VMEM], out_specs=VMEM,
            )(parts)
            col_part = call(
                functools.partial(col_body, total_rows),
                jax.ShapeDtypeStruct((nz, 1, k_own), f32),
                2 * elements, 4 * elements,
                in_specs=[VMEM, VMEM], out_specs=VMEM,
            )(weights, exchange(copies, "y"))
    sent = call(
        last_body, jax.ShapeDtypeStruct((ny, 1, lanes + k_own), f32),
        ny * ny * lanes, 8 * ny * ny * lanes, in_specs=[VMEM, VMEM, pl.BlockSpec(memory_space=pl.ANY)], out_specs=VMEM,
    )(parts, col_scale, in_hbm(every_proto))
    return call(
        functools.partial(targets_body, total_rows),
        jax.ShapeDtypeStruct((n, k_out), bf16),
        2 * elements * dim, 6 * elements,
        in_specs=[VMEM, VMEM, VMEM, VMEM],
        out_specs=pl.BlockSpec(memory_space=pltpu.HBM),
        scratch_shapes=[pltpu.VMEM((ny, n, k_own), bf16), pltpu.SemaphoreType.DMA((ny,))],
    )(mine, mine_scale, every_proto, exchange(sent, "y"))


def solution(mesh):
    rows = mesh.shape["rows"]
    split = Mesh(mesh.devices.reshape(NY, rows // NY, mesh.shape["protos"]), ("y", "z", "p"))
    in_specs = (P(("y", "z"), "p"), P("p", ("y", "z")), P(("y", "z")))
    out_specs = P(("y", "z"), "p")
    return jax.shard_map(
        on_device, mesh=split, in_specs=in_specs, out_specs=out_specs, check_vma=False
    )
```

```python
import functools

import jax
import jax.numpy as jnp
from jax import lax
from jax.experimental import pallas as pl
from jax.experimental.pallas import tpu as pltpu
from jax.sharding import Mesh
from jax.sharding import PartitionSpec as P


K = 65536
ITERS = 3
TEMP = 0.07
EPS = 1e-06
NY = 8
CORES = 2
LANES = 128
VMEM = pl.BlockSpec(memory_space=pltpu.VMEM)


def exchange(value, axes):
    return lax.all_to_all(value, axes, split_axis=0, concat_axis=0, tiled=True)


def in_hbm(value):
    return pltpu.with_memory_space_constraint(value, pltpu.HBM)


def call(body, out_shape, flops, moved, limit=20 * 2**20, **kwargs):
    return pl.pallas_call(
        body,
        out_shape=out_shape,
        cost_estimate=pl.CostEstimate(flops=flops, bytes_accessed=moved, transcendentals=0),
        compiler_params=pltpu.CompilerParams(vmem_limit_bytes=limit),
        **kwargs,
    )


def lane_sums(block, lanes):
    empty = jnp.zeros((lanes - block.shape[0], block.shape[1]), jnp.float32)
    return jnp.sum(jnp.concatenate([block, empty], axis=0).T, axis=0, keepdims=True)


def first_body(features, protos, index, both):
    ny, rows, lanes = both.shape
    share, count = features.shape
    n = index.shape[1]
    index = jnp.concatenate([index[...], jnp.full((1, lanes - n), -1, jnp.int32)], axis=1)
    picks = lax.broadcasted_iota(jnp.int32, (count, lanes), 0) == index
    chosen = lax.dot_general(
        features[...], picks.astype(jnp.float32).astype(jnp.bfloat16),
        (((1,), (0,)), ((), ())), preferred_element_type=jnp.float32,
    ).astype(jnp.bfloat16)
    held = rows - share
    for y in range(ny):
        for at in range(0, held, 2):
            start = (y * held // 2 + at // 2) * lanes
            both[y, at : at + 2, :] = protos[:, start : start + lanes]
        both[y, held:, :] = chosen


def second_body(both, chosen, pieces):
    ny = both.shape[0]
    nz, _, _ = pieces.shape
    lanes = both.shape[2]
    held = both.shape[1] - chosen.shape[1]
    chosen[...] = both[:, held:, :]
    for y in range(ny):
        for at in range(0, held, 2):
            pair = both[y, at : at + 2, :]
            start = at // 2 * lanes
            for z in range(nz):
                pieces[z, 2 * y : 2 * y + 2, start : start + lanes] = pair


def keep_body(protos, kept, sem):
    copy = pltpu.make_async_copy(protos, kept, sem)
    copy.start()
    copy.wait()


def squared_scale(protos):
    wide = protos.astype(jnp.float32)
    return lax.rsqrt(jnp.sum(wide * wide, axis=0, keepdims=True) + EPS)


def block_weights(feat, feat_scale, protos):
    proto_scale = squared_scale(protos)
    raw = lax.dot_general(
        feat, protos, (((1,), (0,)), ((), ())), preferred_element_type=jnp.float32
    )
    parts = []
    for at in range(0, raw.shape[1], LANES):
        part = raw[:, at : at + LANES] * feat_scale * proto_scale[:, at : at + LANES]
        parts.append(jnp.exp(part / TEMP))
    return jnp.concatenate(parts, axis=1)


def arrival_order(ny, nz):
    dim = 2 * ny * nz
    at = lax.broadcasted_iota(jnp.int32, (dim, dim), 0)
    low, mid = at & 1, (at >> 1) & (nz - 1)
    high = at >> nz.bit_length()
    target = mid * (2 * ny) + high * 2 + low
    hit = lax.broadcasted_iota(jnp.int32, (dim, dim), 1) == target
    return hit.astype(jnp.float32).astype(jnp.bfloat16)


def feats_body(nz, ny, me, patches, feats, scales, mine, mine_scale):
    npr, count, share, lanes = patches.shape
    n = feats.shape[1]
    step = pl.program_id(0)
    order = arrival_order(ny, nz)
    for k in range(count):
        y = step * count + k
        feat = patches[:, k].reshape(npr * share, lanes)
        scales[y] = jnp.broadcast_to(squared_scale(feat), (LANES, lanes)).T[:n]
        feats[y] = lax.dot_general(
            feat.T[:n], order, (((1,), (0,)), ((), ())), preferred_element_type=jnp.float32
        ).astype(jnp.bfloat16)

    @pl.when(step == pl.num_programs(0) - 1)
    def _():
        mine[...] = feats[me[0]]
        mine_scale[...] = scales[me[0]]


def weights_body(core, feats, scales, protos, weights, col_part):
    values = protos[...]
    total = jnp.zeros((8, values.shape[1]), jnp.float32)
    for y in range(feats.shape[0]):
        block = block_weights(feats[y], scales[y], values)
        weights[y] = block
        total = total + jnp.sum(block.reshape(-1, 8, block.shape[1]), axis=0)
    total = jnp.sum(total, axis=0, keepdims=True)
    for z in range(col_part.shape[0]):
        col_part[z] = total


def row_body(weights, parts, row_part, col_scale):
    total = parts[0]
    for z in range(1, parts.shape[0]):
        total = total + parts[z]
    scale = 1.0 / (K * total)
    col_scale[...] = scale
    ny, _, width = weights.shape
    for y in range(ny):
        acc = weights[y, :, :LANES] * scale[:, :LANES]
        for at in range(LANES, width, LANES):
            acc = acc + weights[y, :, at : at + LANES] * scale[:, at : at + LANES]
        sums = lane_sums(acc, row_part.shape[2])
        for p in range(row_part.shape[0]):
            row_part[p, y : y + 1, :] = sums


def col_body(total_rows, weights, parts, col_part):
    total = parts[0]
    for y in range(1, parts.shape[0]):
        total = total + parts[y]
    scale = 1.0 / (total_rows * total)
    ny, n, width = weights.shape
    flipped = scale.T
    acc = jnp.zeros((8, width), jnp.float32)
    for y in range(ny):
        block = weights[y] * flipped[:n, y : y + 1]
        acc = acc + jnp.sum(block.reshape(n // 8, 8, width), axis=0)
    total = jnp.sum(acc, axis=0, keepdims=True)
    for z in range(col_part.shape[0]):
        col_part[z] = total


def added(parts):
    total = parts[0]
    for k in range(1, parts.shape[0]):
        total = total + parts[k]
    return total


def relay_body(parts, copies):
    total = added(parts)
    for y in range(copies.shape[0]):
        copies[y] = total


def last_body(core, parts, col_scale, every_proto, sent):
    total = added(parts)
    lanes = total.shape[1]
    pairs = sent.shape[0] // total.shape[0]
    for k in range(sent.shape[0]):
        y = k // pairs
        sent[k, :, :lanes] = total[y : y + 1]
        sent[k, :, lanes:] = col_scale[...]


def targets_body(total_rows, core, mine, mine_scale, protos, got, out, slots, sems):
    count, n, width = slots.shape
    lanes = got.shape[2] - width
    total = got[0, :, :lanes]
    for k in range(1, got.shape[0]):
        total = total + got[k, :, :lanes]
    factor = float(K) * float(total_rows)
    scale = factor * (1.0 / (total_rows * total))
    scale = jnp.broadcast_to(scale, (LANES, lanes)).T[:n]
    copies = []
    for y in range(count):
        block = block_weights(mine[...], mine_scale[...], protos[y])
        col_scale = got[y * (got.shape[0] // count) + core[0]][:, lanes:]
        for at in range(0, width, LANES):
            part = scale * block[:, at : at + LANES] * col_scale[:, at : at + LANES]
            slots[y, :, at : at + LANES] = part.astype(jnp.bfloat16)
        copy = pltpu.make_async_copy(
            slots.at[y], out.at[:, y * width : (y + 1) * width], sems.at[y]
        )
        copy.start()
        copies.append(copy)
    for copy in copies:
        copy.wait()


def on_device(features, prototypes, masked_index):
    n = masked_index.shape[0]
    ny, nz, npr = lax.axis_size("y"), lax.axis_size("z"), lax.axis_size(("x", "c"))
    nx, nc = lax.axis_size("x"), lax.axis_size("c")
    total_rows = n * ny * nz
    k_out = prototypes.shape[0]
    k_own = k_out // ny
    lanes = -(-n // LANES) * LANES
    dim = features.shape[1] * npr
    f32, bf16 = jnp.float32, jnp.bfloat16
    elements = ny * n * k_own

    share = features.shape[1]
    held = 2 * k_own // lanes
    both = call(
        first_body, jax.ShapeDtypeStruct((ny, held + share, lanes), bf16),
        2 * share * lanes * features.shape[0], 4 * ny * share * lanes,
        grid=(1,),
        in_specs=[
            pl.BlockSpec((share, features.shape[0]), lambda i: (0, 0)),
            pl.BlockSpec((2, k_out), lambda i: (0, 0)),
            pl.BlockSpec((1, n), lambda i: (0, 0)),
        ],
        out_specs=VMEM,
    )(in_hbm(features.T), in_hbm(prototypes.T), in_hbm(masked_index.reshape(1, n)))
    both = exchange(both, "y")
    chosen, pieces = call(
        second_body,
        (
            jax.ShapeDtypeStruct((ny, share, lanes), bf16),
            jax.ShapeDtypeStruct((nz, 2 * ny, k_own), bf16),
        ),
        ny * share * lanes, 4 * dim * k_own,
        grid=(1,),
        in_specs=[VMEM],
        out_specs=(
            pl.BlockSpec((ny, share, lanes), lambda i: (0, 0, 0)),
            pl.BlockSpec((nz, 2 * ny, k_own), lambda i: (0, 0, 0)),
        ),
    )(both)
    patches = lax.all_gather(chosen, ("x", "c"))
    protos = exchange(pieces, "z").reshape(dim, k_own)
    prepared = call(
        functools.partial(feats_body, nz, ny),
        (
            jax.ShapeDtypeStruct((ny, n, dim), bf16),
            jax.ShapeDtypeStruct((ny, n, LANES), f32),
            jax.ShapeDtypeStruct((n, dim), bf16),
            jax.ShapeDtypeStruct((n, LANES), f32),
        ),
        2 * ny * lanes * dim, 4 * ny * lanes * dim,
        grid=(2,),
        in_specs=[
            pl.BlockSpec(memory_space=pltpu.SMEM),
            pl.BlockSpec((npr, ny // 2, share, lanes), lambda i: (0, i, 0, 0)),
        ],
        out_specs=(VMEM, VMEM, VMEM, VMEM),
    )(lax.axis_index("y").reshape(1), in_hbm(patches))
    core = lax.axis_index("c").reshape(1)
    feats, scales, mine, mine_scale = prepared
    kept = call(
        keep_body, jax.ShapeDtypeStruct((dim, k_own), bf16), dim * k_own, 4 * dim * k_own,
        in_specs=[VMEM],
        out_specs=pl.BlockSpec(memory_space=pltpu.HBM),
        scratch_shapes=[pltpu.SemaphoreType.DMA],
    )(protos)
    every_proto = lax.all_gather(kept, "y")
    weights, col_part = call(
        weights_body,
        (
            jax.ShapeDtypeStruct((ny, n, k_own), f32),
            jax.ShapeDtypeStruct((nz, 1, k_own), f32),
        ),
        2 * elements * dim, 4 * elements,
        in_specs=[pl.BlockSpec(memory_space=pltpu.SMEM), VMEM, VMEM, VMEM],
        out_specs=(VMEM, VMEM),
    )(core, feats, scales, protos)

    for step in range(ITERS):
        parts = exchange(col_part, "z")
        row_part, col_scale = call(
            row_body,
            (jax.ShapeDtypeStruct((nx, ny, lanes), f32), jax.ShapeDtypeStruct((1, k_own), f32)),
            2 * elements, 4 * elements,
            in_specs=[VMEM, VMEM], out_specs=(VMEM, VMEM),
        )(weights, parts)
        parts = exchange(row_part, "x")
        if step + 1 < ITERS:
            copies = call(
                relay_body, jax.ShapeDtypeStruct((ny * nc, ny, lanes), f32),
                ny * ny * lanes, 8 * ny * ny * lanes, in_specs=[VMEM], out_specs=VMEM,
            )(parts)
            col_part = call(
                functools.partial(col_body, total_rows),
                jax.ShapeDtypeStruct((nz, 1, k_own), f32),
                2 * elements, 4 * elements,
                in_specs=[VMEM, VMEM], out_specs=VMEM,
            )(weights, exchange(copies, ("y", "c")))
    sent = call(
        last_body, jax.ShapeDtypeStruct((ny * nc, 1, lanes + k_own), f32),
        ny * ny * lanes, 8 * ny * ny * lanes, in_specs=[pl.BlockSpec(memory_space=pltpu.SMEM), VMEM, VMEM, pl.BlockSpec(memory_space=pl.ANY)],
        out_specs=VMEM,
    )(core, parts, col_scale, in_hbm(every_proto))
    return call(
        functools.partial(targets_body, total_rows),
        jax.ShapeDtypeStruct((n, k_out), bf16),
        2 * elements * dim, 6 * elements,
        in_specs=[pl.BlockSpec(memory_space=pltpu.SMEM), VMEM, VMEM, VMEM, VMEM],
        out_specs=pl.BlockSpec(memory_space=pltpu.HBM),
        scratch_shapes=[pltpu.VMEM((ny, n, k_own), bf16), pltpu.SemaphoreType.DMA((ny,))],
    )(core, mine, mine_scale, every_proto, exchange(sent, ("y", "c")))


def solution(mesh):
    rows, protos = mesh.shape["rows"], mesh.shape["protos"]
    split = Mesh(
        mesh.devices.reshape(NY, rows // NY, protos // CORES, CORES), ("y", "z", "x", "c"))
    in_specs = (P(("y", "z"), ("x", "c")), P(("x", "c"), ("y", "z")), P(("y", "z")))
    out_specs = P(("y", "z"), ("x", "c"))
    return jax.shard_map(
        on_device, mesh=split, in_specs=in_specs, out_specs=out_specs, check_vma=False
    )
```
